32 devices in a mesh: donor: 4 (over y, x), gene: 8 (over z, core).
Axes of the slice: x: 2, y: 2, z: 4, core: 2. Of those that a mesh axis runs over, the one named last changes fastest.
Arguments:
- partition_tallies: bfloat16 [4096, 40352], P('donor', 'gene'), may hold values from 0 to 4
- blank_tallies: bfloat16 [1024, 40352], P('donor', 'gene'), may hold values from 0 to 1
- cluster_assignment: int32 [4096], P('donor'), may hold values from 0 to 63
- partition_person_label: int32 [4096], P('donor'), may hold values from 0 to 11
- person_blank_members: int32 [12, 384], replicated, may hold values from 0 to 1023
- spillover_fraction: float32 [4096], P('donor'), may hold values from 0.05 to 0.7
- cluster_expression: float32 [64, 40352], P(None, 'gene'), may hold values from 0.05 to 20
- background_profile: float32 [12, 40352], P(None, 'gene'), may hold values from 0.05 to 20
Outputs:
- new_profiles: float32 [64, 40352], P('donor', 'gene')
- new_ambient: float32 [12, 40352], P(None, 'gene')
- new_theta: float32 [4096], P('donor')
- ambient_reads: float32 [4096], P('donor')
The draws below stay inside these ranges and needn't reach their ends.
Inputs may be any that keep to these rules, and one draw needn't show every extreme that they name: `person_blank_members`: an index may be listed more than once.
All inputs are finite; a program needn't handle non-finite values.
Results may differ from the reference program's by a relative error of at most 0.0003.
Values sent between devices are 32-bit elements; how exact they have to be, the bound alone decides.
No kernel may reach another device: no remote copies, remote signals or barrier semaphores. Data moves between devices by JAX's collectives and lax.ppermute only.
A program may use at most 64 MiB of HBM per device.

```python
import math
import jax
import jax.numpy as jnp
from jax import lax

TRANSCRIPT_TOTAL = 40352
POPS = 64
DONOR_NUMBER = 12
CELL_DEV = 1024
LIST_ENTRIES = 384
CELLS = 4096
BLANK_PARTITIONS = 1024
N_DONOR = 4


def touch_ends(entries, rng, smallest, top_value):
    longest = entries.shape.index(max(entries.shape))
    spots = []
    for shift in (0, 1):
        where = [jax.random.randint(jax.random.fold_in(rng, axis), (), 0, length) for axis, length in enumerate(entries.shape)]
        where[longest] = (where[longest] + shift) % entries.shape[longest]
        spots.append(tuple(where))
    return entries.at[spots[0]].set(smallest).at[spots[1]].set(top_value)


def level_of(stream_key, extent, shards, least, top_value):
    gain = 1.0
    for dim, parts in shards:
        heights = jax.random.uniform(jax.random.fold_in(jax.random.fold_in(stream_key, 6), dim), (parts,), jnp.float32, least / len(shards), top_value / len(shards))
        gain = gain * jnp.repeat(jnp.exp(heights), extent[dim] // parts).reshape((-1,) + (1,) * (len(extent) - 1 - dim))
    return gain


def setup_inputs(seed: int = 0) -> dict:
    arg_keys = jax.random.split(jax.random.key(seed), 9)
    return {
        "partition_tallies": jnp.clip(4.0 * jax.random.uniform(arg_keys[0], (CELLS, TRANSCRIPT_TOTAL), jnp.float32) ** level_of(arg_keys[0], (CELLS, TRANSCRIPT_TOTAL), ((0, 4), (1, 8)), -0.2, 0.2), 0.0, 4.0).astype(jnp.bfloat16),
        "blank_tallies": jnp.clip(1.0 * jax.random.uniform(arg_keys[1], (BLANK_PARTITIONS, TRANSCRIPT_TOTAL), jnp.float32) ** level_of(arg_keys[1], (BLANK_PARTITIONS, TRANSCRIPT_TOTAL), ((0, 4), (1, 8)), -0.2, 0.2), 0.0, 1.0).astype(jnp.bfloat16),
        "cluster_assignment": touch_ends(jax.random.randint(arg_keys[2], (CELLS,), 0, POPS), jax.random.fold_in(arg_keys[2], 1), 0, POPS - 1).astype(jnp.int32),
        "partition_person_label": touch_ends(jax.random.randint(arg_keys[3], (CELLS,), 0, DONOR_NUMBER), jax.random.fold_in(arg_keys[3], 1), 0, DONOR_NUMBER - 1).astype(jnp.int32),
        "person_blank_members": touch_ends(jax.random.randint(arg_keys[4], (DONOR_NUMBER, LIST_ENTRIES), 0, BLANK_PARTITIONS), jax.random.fold_in(arg_keys[4], 1), 0, BLANK_PARTITIONS - 1).astype(jnp.int32),
        "spillover_fraction": jnp.clip(0.05 + 0.65 * jax.random.uniform(arg_keys[5], (CELLS,), jnp.float32) ** level_of(arg_keys[5], (CELLS,), ((0, 4),), -0.2, 0.2), 0.05, 0.7),
        "cluster_expression": jnp.clip(jnp.exp(math.log(20.0) - 5.9914645 * jax.random.uniform(arg_keys[6], (POPS, TRANSCRIPT_TOTAL), jnp.float32) ** level_of(arg_keys[6], (POPS, TRANSCRIPT_TOTAL), ((1, 8),), -0.2, 0.2)), 0.05, 20.0),
        "background_profile": jnp.clip(jnp.exp(math.log(20.0) - 5.9914645 * jax.random.uniform(arg_keys[7], (DONOR_NUMBER, TRANSCRIPT_TOTAL), jnp.float32) ** level_of(arg_keys[7], (DONOR_NUMBER, TRANSCRIPT_TOTAL), ((1, 8),), -0.2, 0.2)), 0.05, 20.0),
    }


pseudo_count = 0.5
beta_prior = 10.0


def reference(partition_tallies, blank_tallies, cluster_assignment, partition_person_label, person_blank_members, spillover_fraction, cluster_expression, background_profile):
    def droplet_block(carry, pieces):
        pop_sums, background_transcript_totals = carry
        block_counts, block_labels, block_donors, block_theta = pieces
        weight_native = (1.0 - block_theta[:, None]) * cluster_expression[block_labels]
        weight_contam = block_theta[:, None] * background_profile[block_donors]
        resp_native = weight_native / (weight_native + weight_contam)
        count_values = block_counts.astype(jnp.float32)
        native = (count_values * resp_native).astype(jnp.bfloat16).astype(jnp.float32)
        contam = (count_values * (1.0 - resp_native)).astype(jnp.bfloat16).astype(jnp.float32)
        pop_hot = (block_labels[:, None] == jnp.arange(POPS, dtype=jnp.int32)[None, :]).astype(jnp.float32)
        donor_hot = (block_donors[:, None] == jnp.arange(DONOR_NUMBER, dtype=jnp.int32)[None, :]).astype(jnp.float32)
        pop_sums = pop_sums + jnp.dot(pop_hot.T, native, precision=lax.Precision.HIGHEST)
        background_transcript_totals = background_transcript_totals + jnp.dot(donor_hot.T, contam, precision=lax.Precision.HIGHEST)
        return (pop_sums, background_transcript_totals), (jnp.sum(native, axis=1), jnp.sum(contam, axis=1))

    start = (jnp.zeros((POPS, TRANSCRIPT_TOTAL), jnp.float32), jnp.zeros((DONOR_NUMBER, TRANSCRIPT_TOTAL), jnp.float32))
    pieces = (partition_tallies.reshape(N_DONOR, CELL_DEV, TRANSCRIPT_TOTAL), cluster_assignment.reshape(N_DONOR, CELL_DEV),
              partition_person_label.reshape(N_DONOR, CELL_DEV), spillover_fraction.reshape(N_DONOR, CELL_DEV))
    (pop_sums, background_transcript_totals), (native_reads, contam_reads) = lax.scan(droplet_block, start, pieces)
    native_reads = native_reads.reshape(CELLS)
    contam_reads = contam_reads.reshape(CELLS)
    gathered_blank_tallies = jnp.sum((person_blank_members[:, :, None] == jnp.arange(BLANK_PARTITIONS, dtype=jnp.int32)[None, None, :]).astype(jnp.float32), axis=1)
    background_transcript_totals = background_transcript_totals + jnp.dot(gathered_blank_tallies, blank_tallies.astype(jnp.float32), precision=lax.Precision.HIGHEST)
    new_profiles = TRANSCRIPT_TOTAL * (pop_sums + pseudo_count) / (jnp.sum(pop_sums, axis=1)[:, None] + TRANSCRIPT_TOTAL * pseudo_count)
    new_ambient = TRANSCRIPT_TOTAL * (background_transcript_totals + pseudo_count) / (jnp.sum(background_transcript_totals, axis=1)[:, None] + TRANSCRIPT_TOTAL * pseudo_count)
    new_theta = (contam_reads + beta_prior) / (native_reads + contam_reads + 2.0 * beta_prior)
    ambient_reads = contam_reads / TRANSCRIPT_TOTAL
    return new_profiles, new_ambient, new_theta, ambient_reads
```

```python
import functools

import jax
import jax.numpy as jnp
from jax import lax
from jax.experimental import pallas as pl
from jax.experimental.pallas import tpu as pltpu
from jax.sharding import PartitionSpec as P

TRANSCRIPT_TOTAL = 40352
PSEUDO = 0.5
BETA = 10.0
LANES = 128
SHARES = (5, 5, 5, 5)


def up(value, step):
    return -(-value // step) * step


def three(value):
    high = value.astype(jnp.bfloat16)
    rest = value - high.astype(jnp.float32)
    mid = rest.astype(jnp.bfloat16)
    low = (rest - mid.astype(jnp.float32)).astype(jnp.bfloat16)
    return high, mid, low


def pad_rows(value, rows):
    short = rows - value.shape[0]
    if not short:
        return value
    return jnp.concatenate([value, jnp.zeros((short, value.shape[1]), value.dtype)], axis=0)


def prep_kernel(pops, donors, me_ref, label_ref, person_ref, theta_ref, hot_ref, pop_ref, person_hot_ref):
    cells = label_ref.shape[1]
    donor_rows = person_hot_ref.shape[0]
    share = pops // me_ref[1]
    label = label_ref[...]
    person = person_ref[...]
    pop_iota = lax.broadcasted_iota(jnp.int32, (pops, cells), 0)
    donor_iota = lax.broadcasted_iota(jnp.int32, (donor_rows, cells), 0)
    one = lambda mask: jnp.where(mask, 1.0, 0.0).astype(jnp.bfloat16)
    pop_hot = one(label == pop_iota)
    person_hot = one(person == donor_iota)
    theta = theta_ref[...]
    ratio = (0.5 * (jnp.log(1.0 - theta) - jnp.log(theta))).astype(jnp.float32)
    parts = [part.astype(jnp.float32) for part in three(ratio)]
    row = lax.broadcasted_iota(jnp.int32, (16, cells), 0)
    extra = jnp.where(row == 0, parts[0], jnp.where(row == 1, parts[1], jnp.where(row == 2, parts[2], 0.0)))
    stacked = jnp.concatenate([pop_hot] * 3 + [person_hot] * 3 + [extra.astype(jnp.bfloat16)], axis=0)
    hot_ref[...] = stacked.T
    pop_ref[...] = one((label ^ (me_ref[0] * share)) == pop_iota)
    person_hot_ref[...] = person_hot


def group_kernel(
    first, limit, masked, order, share, steps,
    hot_ref, pop_ref, person_ref, listed_ref, ca_ref, cb_ref, ba_ref, bb_ref, ea_ref, eb_ref, pa_ref, pb_ref,
    send_ref, keep_ref, reads_ref, totals_ref, native_acc, contam_acc,
):
    step = pl.program_id(0)
    cells = hot_ref.shape[0]
    pops = pop_ref.shape[0]
    donor_rows = person_ref.shape[0]
    donors = pa_ref.shape[0]

    @pl.when(step == 0)
    def _():
        native_acc[...] = jnp.zeros_like(native_acc)
        contam_acc[...] = jnp.zeros_like(contam_acc)
        totals_ref[...] = jnp.zeros_like(totals_ref)

    def joined(a_ref, b_ref, fill):
        value = jnp.concatenate([a_ref[...], b_ref[...]], axis=1)
        if not masked:
            return value
        lane = lax.broadcasted_iota(jnp.int32, (1, 2 * LANES), 1)
        column = first + step * LANES + jnp.where(lane < LANES, lane, lane - LANES + steps * LANES)
        return jnp.where(column < limit, value, jnp.asarray(fill, value.dtype))

    logs = 0.5 * jnp.log(joined(ea_ref, eb_ref, 1.0))
    person_logs = pad_rows(-0.5 * jnp.log(joined(pa_ref, pb_ref, 1.0)), donor_rows)
    extra = jnp.where(lax.broadcasted_iota(jnp.int32, (16, 2 * LANES), 0) < 3, 1.0, 0.0).astype(jnp.bfloat16)
    table = jnp.concatenate(list(three(logs)) + list(three(person_logs)) + [extra], axis=0)
    blanks = joined(ba_ref, bb_ref, 0.0)
    counts = joined(ca_ref, cb_ref, 0.0)

    listed = jnp.dot(listed_ref[...], blanks, preferred_element_type=jnp.float32)
    ambient = listed[:donor_rows] + listed[donor_rows:]
    pop = jnp.zeros((pops, 2 * LANES), jnp.float32)
    block = min(cells, 256)
    for at in range(0, cells, block):
        rows = slice(at, at + block)
        logit = jnp.dot(hot_ref[rows, :], table, preferred_element_type=jnp.float32)
        lean = jnp.tanh(logit)
        count = counts[rows, :].astype(jnp.float32)
        tilt = count * lean
        native = (count + tilt).astype(jnp.bfloat16)
        contam = (count - tilt).astype(jnp.bfloat16)
        pop += jnp.dot(pop_ref[:, rows], native, preferred_element_type=jnp.float32)
        ambient += jnp.dot(person_ref[:, rows], contam, preferred_element_type=jnp.float32)
        native_wide = native.astype(jnp.float32)
        contam_wide = contam.astype(jnp.float32)
        native_acc[rows, :] += native_wide[:, :LANES] + native_wide[:, LANES:]
        contam_acc[rows, :] += contam_wide[:, :LANES] + contam_wide[:, LANES:]
    pop = 0.5 * pop
    ambient = 0.5 * ambient

    totals_ref[:pops, :] += pop[:, :LANES] + pop[:, LANES:]
    totals_ref[pops:, :] += ambient[:, :LANES] + ambient[:, LANES:]
    half = len(order) // 2
    for ref, blocks in ((keep_ref, order[:half]), (send_ref, order[half:])):
        for place, which in enumerate(blocks):
            for side in range(2):
                at = (2 * place + side) * share
                ref[at : at + share, :] = pop[which * share : (which + 1) * share, side * LANES : (side + 1) * LANES]
        at = 2 * half * share
        ref[at : at + donors, :] = ambient[:donors, :LANES]
        ref[at + donors : at + 2 * donors, :] = ambient[:donors, LANES:]

    @pl.when(step == steps - 1)
    def _():
        ones = jnp.ones((8, LANES), jnp.float32)
        for at, acc in ((0, native_acc), (1, contam_acc)):
            row = lax.dot_general(
                ones, acc[...], (((1,), (1,)), ((), ())),
                precision=lax.Precision.HIGHEST, preferred_element_type=jnp.float32,
            )
            reads_ref[at : at + 1, :] = 0.5 * row[:1, :]


def stats_kernel(pops, share, count, me_ref, *refs):
    reads, totals, out_ref = refs[:count], refs[count : 2 * count], refs[2 * count]
    cells = reads[0].shape[1]
    total = totals[0][...]
    read = reads[0][...]
    for part in totals[1:]:
        total = total + part[...]
    for part in reads[1:]:
        read = read + part[...]
    lines = cells // LANES
    for which in range(2):
        for line in range(lines):
            out_ref[which * lines + line : which * lines + line + 1, :] = read[which : which + 1, line * LANES : (line + 1) * LANES]
    column = jnp.sum(total, axis=1, keepdims=True)
    row = lax.broadcasted_iota(jnp.int32, total.shape, 0)
    lane = lax.broadcasted_iota(jnp.int32, total.shape, 1)
    goal = jnp.where(row < pops, row ^ (me_ref[0] * share), row)
    line = jnp.sum(jnp.where(lane == goal, column, 0.0), axis=0, keepdims=True)
    out_ref[2 * lines : 2 * lines + 8, :] = jnp.broadcast_to(line, (8, LANES))


def final_kernel(pops, share, donors, widths, limit, count, me_ref, tot_ref, *refs):
    sums, last, profile_ref, ambient_ref = refs[:count], refs[count : 2 * count], refs[2 * count], refs[2 * count + 1]
    total = tot_ref[:1, :]

    def column(rows, base):
        row = lax.broadcasted_iota(jnp.int32, (rows, LANES), 0)
        lane = lax.broadcasted_iota(jnp.int32, (rows, LANES), 1)
        value = jnp.sum(jnp.where(lane == row + base, total, 0.0), axis=1, keepdims=True)
        return value + TRANSCRIPT_TOTAL * PSEUDO

    pop_scale = column(share, me_ref[0] * share)
    ambient_scale = column(donors, pops)
    at = 0
    for group in range(count):
        width = widths[group]
        kept = sums[group].shape[0] - 2 * donors
        own = 2 * share
        for side in range(2):
            begin = at + side * width
            size = min(width, limit - begin)
            if size <= 0:
                continue
            rows = slice(side * share, (side + 1) * share)
            value = sums[group][rows, :size] + last[group][rows, :size]
            profile_ref[:, begin : begin + size] = TRANSCRIPT_TOTAL * (value + PSEUDO) / pop_scale
            here = kept + side * donors
            there = own + side * donors
            value = sums[group][here : here + donors, :size] + last[group][there : there + donors, :size]
            ambient_ref[:, begin : begin + size] = TRANSCRIPT_TOTAL * (value + PSEUDO) / ambient_scale
        at += 2 * width


def split(units, shares):
    total, seen, sizes, done = sum(shares), 0, [], 0
    for share in shares:
        seen += share
        size = units * seen // total - done
        if size:
            sizes.append(size)
        done += size
    return sizes


def swap(value, axis, size, bit):
    return lax.ppermute(value, axis, [(index, index ^ bit) for index in range(size)])


def solution(mesh):
    n_donor, n_gene = mesh.shape["donor"], mesh.shape["gene"]
    donor_bits = [1 << b for b in range(n_donor.bit_length() - 1)]
    gene_bits = [1 << b for b in range(n_gene.bit_length() - 1)]
    assert 1 << len(donor_bits) == n_donor and 1 << len(gene_bits) == n_gene

    def body(tallies, blanks, label, person, members, theta, expression, background):
        cells, genes = tallies.shape
        empties = blanks.shape[0]
        pops, donors = expression.shape[0], background.shape[0]
        donor_rows = up(donors, 16)
        share = pops // n_donor
        depth = 3 * pops + 3 * donor_rows + 16
        whole = lambda shape: pl.BlockSpec(shape, lambda i: (0,) * len(shape))
        vmem = pl.BlockSpec(memory_space=pltpu.VMEM)
        smem = pl.BlockSpec(memory_space=pltpu.SMEM)
        bf16, f32 = jnp.bfloat16, jnp.float32

        index = lax.axis_index("donor")
        me = jnp.stack([index, jnp.int32(n_donor)]).astype(jnp.int32)
        local = index * empties + jnp.arange(empties, dtype=jnp.int32)
        times = jnp.sum((members[:, :, None] == local[None, None, :]).astype(f32), axis=1)
        low = jnp.minimum(times, 256.0)
        spare = ((0, donor_rows - donors), (0, 0))
        listed = (2.0 * jnp.concatenate([jnp.pad(low, spare), jnp.pad(times - low, spare)])).astype(bf16)

        def prep(me_ref, *refs):
            me_pair = (me_ref[0], n_donor)
            prep_kernel(pops, donors, me_pair, *refs)

        hot, pop_hot, person_hot = pl.pallas_call(
            prep,
            out_shape=(
                jax.ShapeDtypeStruct((cells, depth), bf16),
                jax.ShapeDtypeStruct((pops, cells), bf16),
                jax.ShapeDtypeStruct((donor_rows, cells), bf16),
            ),
            in_specs=[smem, vmem, vmem, vmem],
            out_specs=(vmem, vmem, vmem),
            name="prep",
        )(me, label.reshape(1, cells), person.reshape(1, cells), theta.reshape(1, cells))

        blocks = -(-genes // LANES)
        sizes = split(-(-blocks // 2), SHARES)
        keeps, sends, reads, totals, bit_orders = [], [], [], [], []
        start = 0
        for group, steps in enumerate(sizes):
            turn = group % max(len(donor_bits), 1)
            bits = donor_bits[turn:] + donor_bits[:turn]
            bit_orders.append(bits)
            order = [0]
            for bit in reversed(bits):
                order = order + [which | bit for which in order]
            a = functools.partial(lambda base, i: (0, jnp.minimum(base + i, blocks - 1)), start)
            b = functools.partial(lambda base, i: (0, jnp.minimum(base + i, blocks - 1)), start + steps)
            masked = (start + 2 * steps) * LANES > genes
            rows = pops + 2 * donors
            width = steps * LANES
            kernel = functools.partial(group_kernel, start * LANES, genes, masked, tuple(order), share, steps)
            keep_send = jax.ShapeDtypeStruct((rows, width), f32)
            send, keep, read, total = pl.pallas_call(
                kernel,
                grid=(steps,),
                out_shape=(
                    keep_send, keep_send,
                    jax.ShapeDtypeStruct((2, cells), f32),
                    jax.ShapeDtypeStruct((pops + donor_rows, LANES), f32),
                ),
                in_specs=[
                    whole((cells, depth)), whole((pops, cells)), whole((donor_rows, cells)), whole((2 * donor_rows, empties)),
                    pl.BlockSpec((cells, LANES), a), pl.BlockSpec((cells, LANES), b),
                    pl.BlockSpec((empties, LANES), a), pl.BlockSpec((empties, LANES), b),
                    pl.BlockSpec((pops, LANES), a), pl.BlockSpec((pops, LANES), b),
                    pl.BlockSpec((donors, LANES), a), pl.BlockSpec((donors, LANES), b),
                ],
                out_specs=(
                    pl.BlockSpec((rows, LANES), lambda i: (0, i)), pl.BlockSpec((rows, LANES), lambda i: (0, i)),
                    whole((2, cells)), whole((pops + donor_rows, LANES)),
                ),
                scratch_shapes=[pltpu.VMEM((cells, LANES), f32), pltpu.VMEM((cells, LANES), f32)],
                compiler_params=pltpu.CompilerParams(
                    dimension_semantics=("arbitrary",), vmem_limit_bytes=24 * 1024 * 1024
                ),
                cost_estimate=pl.CostEstimate(
                    flops=2 * cells * (depth + pops + donor_rows) * 2 * width,
                    bytes_accessed=2 * (cells + empties) * 2 * width, transcendentals=cells * 2 * width,
                ),
                name=f"group{group}",
            )(hot, pop_hot, person_hot, listed, tallies, tallies, blanks, blanks,
              expression, expression, background, background)
            keeps.append(keep)
            sends.append(send)
            reads.append(read)
            totals.append(total)
            start += 2 * steps

        count = len(sizes)
        for phase in range(len(donor_bits)):
            got = [swap(sends[g], "donor", n_donor, bit_orders[g][phase]) for g in range(count)]
            if phase == len(donor_bits) - 1:
                last = got
            else:
                keeps = [keeps[g] + got[g] for g in range(count)]
                cut = pops // 2 >> phase
                sends = [keep[cut:] for keep in keeps]
                keeps = [jnp.concatenate([keep[:cut], keep[2 * cut :]]) if phase < len(donor_bits) - 2 else keep for keep in keeps]

        lines = 2 * cells // LANES
        message = pl.pallas_call(
            functools.partial(stats_kernel, pops, share, count),
            out_shape=jax.ShapeDtypeStruct((lines + 8, LANES), f32),
            in_specs=[smem] + [vmem] * (2 * count),
            out_specs=vmem,
            name="stats",
        )(me, *reads, *totals)
        for bit in gene_bits:
            message = message + swap(message, "gene", n_gene, bit)
        tot = message[lines:]
        for bit in donor_bits:
            tot = tot + swap(tot, "donor", n_donor, bit)

        native_reads = message[: lines // 2].reshape(cells)
        contam_reads = message[lines // 2 : lines].reshape(cells)
        new_theta = (contam_reads + BETA) / (native_reads + contam_reads + 2.0 * BETA)
        ambient_reads = contam_reads / TRANSCRIPT_TOTAL

        widths = tuple(size * LANES for size in sizes)
        new_profiles, new_ambient = pl.pallas_call(
            functools.partial(final_kernel, pops, share, donors, widths, genes, count),
            out_shape=(
                jax.ShapeDtypeStruct((share, genes), f32),
                jax.ShapeDtypeStruct((donors, genes), f32),
            ),
            in_specs=[smem, vmem] + [vmem] * (2 * count),
            out_specs=(vmem, vmem),
            name="final",
        )(me, tot, *keeps, *last)
        return new_profiles, new_ambient, new_theta, ambient_reads

    in_specs = (
        P("donor", "gene"), P("donor", "gene"), P("donor"), P("donor"), P(), P("donor"),
        P(None, "gene"), P(None, "gene"),
    )
    out_specs = (P("donor", "gene"), P(None, "gene"), P("donor"), P("donor"))
    return jax.shard_map(body, mesh=mesh, in_specs=in_specs, out_specs=out_specs, check_vma=False)
```

```python
import functools

import jax
import jax.numpy as jnp
from jax import lax
from jax.experimental import pallas as pl
from jax.experimental.pallas import tpu as pltpu
from jax.sharding import PartitionSpec as P

TRANSCRIPT_TOTAL = 40352
PSEUDO = 0.5
BETA = 10.0
LANES = 128
TILE = 256
ROWS = 32
SHARES = (2, 2, 3, 3)
MEBI = 1024 * 1024


def up(value, step):
    return -(-value // step) * step


def three(value):
    high = value.astype(jnp.bfloat16)
    rest = value - high.astype(jnp.float32)
    mid = rest.astype(jnp.bfloat16)
    low = (rest - mid.astype(jnp.float32)).astype(jnp.bfloat16)
    return high, mid, low


def pad_rows(value, rows):
    short = rows - value.shape[0]
    if not short:
        return value
    return jnp.concatenate([value, jnp.zeros((short, value.shape[1]), value.dtype)], axis=0)


def prep_kernel(pops, donors, n_donor, label_ref, person_ref, theta_ref, member_ref, hot_ref, pop_ref, person_hot_ref, listed_ref):
    cells = label_ref.shape[1]
    donor_rows = person_hot_ref.shape[0]
    empties = listed_ref.shape[1]
    me = lax.axis_index("donor")
    share = pops // n_donor
    label = label_ref[...]
    person = person_ref[...]
    pop_iota = lax.broadcasted_iota(jnp.int32, (pops, cells), 0)
    donor_iota = lax.broadcasted_iota(jnp.int32, (donor_rows, cells), 0)
    one = lambda mask: jnp.where(mask, 1.0, 0.0).astype(jnp.bfloat16)
    pop_hot = one(label == pop_iota)
    person_hot = one(person == donor_iota)
    theta = theta_ref[...]
    ratio = 0.5 * (jnp.log(1.0 - theta) - jnp.log(theta))
    parts = [part.astype(jnp.float32) for part in three(ratio)]
    row = lax.broadcasted_iota(jnp.int32, (16, cells), 0)
    extra = jnp.where(row == 0, parts[0], jnp.where(row == 1, parts[1], jnp.where(row == 2, parts[2], 0.0)))
    for part in range(3):
        hot_ref[part * pops : (part + 1) * pops, :] = pop_hot
        at = 3 * pops + part * donor_rows
        hot_ref[at : at + donor_rows, :] = person_hot
    hot_ref[3 * pops + 3 * donor_rows :, :] = extra.astype(jnp.bfloat16)
    pop_ref[...] = one((label ^ (me * share)) == pop_iota)
    person_hot_ref[...] = person_hot

    members = member_ref[...].astype(jnp.float32)
    members = pad_rows(members, donor_rows).T
    local = (me * empties + lax.broadcasted_iota(jnp.int32, (1, empties), 1)).astype(jnp.float32)
    listed_ref[...] = jnp.zeros_like(listed_ref)
    for donor in range(donors):
        same = jnp.where(members[:, donor : donor + 1] == local, 1.0, 0.0)
        times = jnp.sum(same, axis=0, keepdims=True)
        low = jnp.minimum(times, 256.0)
        listed_ref[donor : donor + 1, :] = 2.0 * low
        listed_ref[donor_rows + donor : donor_rows + donor + 1, :] = 2.0 * (times - low)


def group_kernel(
    first, limit, order, share, steps,
    hot_ref, pop_ref, person_ref, listed_ref, ca_ref, cb_ref, ba_ref, bb_ref, ea_ref, eb_ref, pa_ref, pb_ref,
    send_ref, keep_ref, reads_ref, totals_ref, *scratch,
):
    step = pl.program_id(0)
    cells = hot_ref.shape[1]
    pops = pop_ref.shape[0]
    donor_rows = person_ref.shape[0]
    donors = pa_ref.shape[0]
    logits, natives, contams = scratch[:2], scratch[2:4], scratch[4:6]
    last_contract = (((1,), (1,)), ((), ()))

    @pl.when(step == 0)
    def _():
        reads_ref[...] = jnp.zeros_like(reads_ref)
        totals_ref[...] = jnp.zeros_like(totals_ref)

    ones = jnp.where(lax.broadcasted_iota(jnp.int32, (16, TILE), 0) < 3, 1.0, 0.0).astype(jnp.bfloat16)
    listed = listed_ref[...].astype(jnp.bfloat16)
    half = len(order) // 2
    sides = ((ca_ref, ba_ref, ea_ref, pa_ref), (cb_ref, bb_ref, eb_ref, pb_ref))
    tables, masks, pop, ambient = [], [], [], []
    for side, (count_ref, blank_ref, native_ref, ambient_ref) in enumerate(sides):
        begin = first + (step + side * steps) * TILE
        masked = first + (side + 1) * steps * TILE > limit
        expression, background = native_ref[...], ambient_ref[...]
        blanks = blank_ref[...]
        if masked:
            column = begin + lax.broadcasted_iota(jnp.int32, (1, TILE), 1)
            expression = jnp.where(column < limit, expression, 1.0)
            background = jnp.where(column < limit, background, 1.0)
            row = begin + lax.broadcasted_iota(jnp.int32, (TILE, LANES), 0)
            masks.append(row < limit)
            wide = begin + lax.broadcasted_iota(jnp.int32, blanks.shape, 0)
            blanks = jnp.where(wide < limit, blanks.astype(jnp.float32), 0.0).astype(jnp.bfloat16)
        else:
            masks.append(None)
        logs = 0.5 * jnp.log(expression)
        person_logs = pad_rows(-0.5 * jnp.log(background), donor_rows)
        table = jnp.concatenate(list(three(logs)) + list(three(person_logs)) + [ones], axis=0)
        tables.append(table.T)
        both = lax.dot_general(listed, blanks, last_contract, preferred_element_type=jnp.float32)
        ambient.append(both[:donor_rows] + both[donor_rows:])
        pop.append(jnp.zeros((pops, TILE), jnp.float32))

    tiles = [(side, at) for side in range(2) for at in range(0, cells, TILE)]

    def look(index):
        side, at = tiles[index]
        logits[index % 2][...] = jnp.dot(tables[side], hot_ref[:, at : at + TILE], preferred_element_type=jnp.float32)

    def weigh(index):
        side, at = tiles[index]
        count_ref = sides[side][0]
        native_sum = jnp.zeros((8, TILE), jnp.float32)
        contam_sum = jnp.zeros((8, TILE), jnp.float32)
        for row in range(0, TILE, ROWS):
            rows = slice(row, row + ROWS)
            lean = jnp.tanh(logits[index % 2][rows, :])
            count = count_ref[rows, at : at + TILE].astype(jnp.float32)
            if masks[side] is not None:
                mask = masks[side][rows, :]
                count = jnp.where(jnp.concatenate([mask] * (TILE // LANES), axis=1), count, 0.0)
            tilt = count * lean
            native = (count + tilt).astype(jnp.bfloat16)
            contam = (count - tilt).astype(jnp.bfloat16)
            natives[index % 2][rows, :] = native
            contams[index % 2][rows, :] = contam
            native_sum += jnp.sum(native.astype(jnp.float32).reshape(ROWS // 8, 8, TILE), axis=0)
            contam_sum += jnp.sum(contam.astype(jnp.float32).reshape(ROWS // 8, 8, TILE), axis=0)
        reads_ref[:8, at : at + TILE] += native_sum
        reads_ref[8:, at : at + TILE] += contam_sum

    def gather(index):
        side, at = tiles[index]
        pop[side] += lax.dot_general(
            pop_ref[:, at : at + TILE], natives[index % 2][...], last_contract, preferred_element_type=jnp.float32
        )
        ambient[side] += lax.dot_general(
            person_ref[:, at : at + TILE], contams[index % 2][...], last_contract, preferred_element_type=jnp.float32
        )

    look(0)
    for index in range(len(tiles)):
        if index + 1 < len(tiles):
            look(index + 1)
        if index:
            gather(index - 1)
        weigh(index)
    gather(len(tiles) - 1)

    for side in range(2):
        total_pop = 0.5 * pop[side]
        total_ambient = 0.5 * ambient[side]
        for at in range(0, TILE, LANES):
            totals_ref[:pops, :] += total_pop[:, at : at + LANES]
            totals_ref[pops:, :] += total_ambient[:, at : at + LANES]
        for ref, blocks in ((keep_ref, order[:half]), (send_ref, order[half:])):
            for place, which in enumerate(blocks):
                at = (2 * place + side) * share
                ref[at : at + share, :] = total_pop[which * share : (which + 1) * share, :]
            at = 2 * half * share + side * donors
            ref[at : at + donors, :] = total_ambient[:donors, :]


def stats_kernel(pops, share, count, *refs):
    reads, totals, out_ref = refs[:count], refs[count : 2 * count], refs[2 * count]
    cells = reads[0].shape[1]
    total = totals[0][...]
    read = reads[0][...]
    for part in totals[1:]:
        total = total + part[...]
    for part in reads[1:]:
        read = read + part[...]
    lines = cells // LANES
    for which in range(2):
        flat = 0.5 * jnp.sum(read[8 * which : 8 * which + 8, :], axis=0, keepdims=True)
        for line in range(lines):
            at = which * lines + line
            out_ref[at : at + 1, :] = flat[:, line * LANES : (line + 1) * LANES]
    column = jnp.sum(total, axis=1, keepdims=True)
    row = lax.broadcasted_iota(jnp.int32, total.shape, 0)
    lane = lax.broadcasted_iota(jnp.int32, total.shape, 1)
    goal = jnp.where(row < pops, row ^ (lax.axis_index("donor") * share), row)
    line = jnp.sum(jnp.where(lane == goal, column, 0.0), axis=0, keepdims=True)
    out_ref[2 * lines : 2 * lines + 8, :] = jnp.broadcast_to(line, (8, LANES))


def final_kernel(pops, share, donors, widths, limit, count, tot_ref, *refs):
    sums, last, profile_ref, ambient_ref = refs[:count], refs[count : 2 * count], refs[2 * count], refs[2 * count + 1]
    total = tot_ref[:1, :]

    def column(rows, base):
        row = lax.broadcasted_iota(jnp.int32, (rows, LANES), 0)
        lane = lax.broadcasted_iota(jnp.int32, (rows, LANES), 1)
        value = jnp.sum(jnp.where(lane == row + base, total, 0.0), axis=1, keepdims=True)
        return value + TRANSCRIPT_TOTAL * PSEUDO

    pop_scale = column(share, lax.axis_index("donor") * share)
    ambient_scale = column(donors, pops)
    at = 0
    for group in range(count):
        width = widths[group]
        kept = sums[group].shape[0] - 2 * donors
        own = 2 * share
        for side in range(2):
            begin = at + side * width
            size = min(width, limit - begin)
            if size <= 0:
                continue
            rows = slice(side * share, (side + 1) * share)
            value = sums[group][rows, :size] + last[group][rows, :size]
            profile_ref[:, begin : begin + size] = TRANSCRIPT_TOTAL * (value + PSEUDO) / pop_scale
            here = kept + side * donors
            there = own + side * donors
            value = sums[group][here : here + donors, :size] + last[group][there : there + donors, :size]
            ambient_ref[:, begin : begin + size] = TRANSCRIPT_TOTAL * (value + PSEUDO) / ambient_scale
        at += 2 * width


def split(units, shares):
    total, seen, sizes, done = sum(shares), 0, [], 0
    for share in shares:
        seen += share
        size = units * seen // total - done
        if size:
            sizes.append(size)
        done += size
    return sizes


def swap(value, axis, size, bit):
    return lax.ppermute(value, axis, [(index, index ^ bit) for index in range(size)])


def solution(mesh):
    n_donor, n_gene = mesh.shape["donor"], mesh.shape["gene"]
    donor_bits = [1 << b for b in range(n_donor.bit_length() - 1)]
    gene_bits = [1 << b for b in range(n_gene.bit_length() - 1)]
    assert 1 << len(donor_bits) == n_donor and 1 << len(gene_bits) == n_gene

    def body(tallies, blanks, label, person, members, theta, expression, background):
        cells, genes = tallies.shape
        empties = blanks.shape[0]
        pops, donors = expression.shape[0], background.shape[0]
        donor_rows = up(donors, 16)
        share = pops // n_donor
        depth = 3 * pops + 3 * donor_rows + 16
        whole = lambda shape: pl.BlockSpec(shape, lambda i: (0,) * len(shape))
        vmem = pl.BlockSpec(memory_space=pltpu.VMEM)
        bf16, f32 = jnp.bfloat16, jnp.float32

        small = lambda mebi: pltpu.CompilerParams(vmem_limit_bytes=mebi * MEBI)
        far = lambda value: pltpu.with_memory_space_constraint(value, pltpu.HBM)
        hot, pop_hot, person_hot, listed = pl.pallas_call(
            functools.partial(prep_kernel, pops, donors, n_donor),
            out_shape=(
                jax.ShapeDtypeStruct((depth, cells), bf16),
                jax.ShapeDtypeStruct((pops, cells), bf16),
                jax.ShapeDtypeStruct((donor_rows, cells), bf16),
                jax.ShapeDtypeStruct((2 * donor_rows, empties), f32),
            ),
            grid=(1,),
            in_specs=[whole((1, cells))] * 3 + [whole(members.shape)],
            out_specs=(vmem, vmem, vmem, vmem),
            compiler_params=small(8),
            name="prep",
        )(far(label.reshape(1, cells)), far(person.reshape(1, cells)), far(theta.reshape(1, cells)), far(members))

        counts, spares, expression, background = far(tallies.T), far(blanks.T), far(expression), far(background)
        blocks = -(-genes // TILE)
        sizes = split(-(-blocks // 2), SHARES)
        keeps, sends, reads, totals, bit_orders = [], [], [], [], []
        start = 0
        for group, steps in enumerate(sizes):
            turn = group % max(len(donor_bits), 1)
            bits = donor_bits[turn:] + donor_bits[:turn]
            bit_orders.append(bits)
            order = [0]
            for bit in reversed(bits):
                order = order + [which | bit for which in order]
            spot = lambda base, i: jnp.minimum(base + i, blocks - 1)
            sides = [functools.partial(spot, base) for base in (start, start + steps)]
            down = lambda rows: [pl.BlockSpec((TILE, rows), functools.partial(lambda at, i: (at(i), 0), at)) for at in sides]
            along = lambda rows: [pl.BlockSpec((rows, TILE), functools.partial(lambda at, i: (0, at(i)), at)) for at in sides]
            rows = pops + 2 * donors
            width = steps * TILE
            kernel = functools.partial(group_kernel, start * TILE, genes, tuple(order), share, steps)
            keep_send = jax.ShapeDtypeStruct((rows, width), f32)
            send, keep, read, total = pl.pallas_call(
                kernel,
                grid=(steps,),
                out_shape=(
                    keep_send, keep_send,
                    jax.ShapeDtypeStruct((16, cells), f32),
                    jax.ShapeDtypeStruct((pops + donor_rows, LANES), f32),
                ),
                in_specs=[vmem] * 4 + down(cells) + down(empties) + along(pops) + along(donors),
                out_specs=(
                    pl.BlockSpec((rows, TILE), lambda i: (0, i)), pl.BlockSpec((rows, TILE), lambda i: (0, i)),
                    whole((16, cells)), whole((pops + donor_rows, LANES)),
                ),
                scratch_shapes=[pltpu.VMEM((TILE, TILE), f32)] * 2 + [pltpu.VMEM((TILE, TILE), bf16)] * 4,
                compiler_params=pltpu.CompilerParams(
                    dimension_semantics=("arbitrary",), vmem_limit_bytes=16 * MEBI
                ),
                cost_estimate=pl.CostEstimate(
                    flops=2 * cells * (depth + pops + donor_rows) * 2 * width,
                    bytes_accessed=2 * (cells + empties) * 2 * width, transcendentals=cells * 2 * width,
                ),
                name=f"group{group}",
            )(hot, pop_hot, person_hot, listed, counts, counts, spares, spares,
              expression, expression, background, background)
            keeps.append(keep)
            sends.append(send)
            reads.append(read)
            totals.append(total)
            start += 2 * steps

        count = len(sizes)
        for phase in range(len(donor_bits)):
            got = [swap(sends[g], "donor", n_donor, bit_orders[g][phase]) for g in range(count)]
            if phase == len(donor_bits) - 1:
                last = got
            else:
                keeps = [keeps[g] + got[g] for g in range(count)]
                cut = pops // 2 >> phase
                sends = [keep[cut:] for keep in keeps]
                keeps = [jnp.concatenate([keep[:cut], keep[2 * cut :]]) if phase < len(donor_bits) - 2 else keep for keep in keeps]

        lines = 2 * cells // LANES
        message = pl.pallas_call(
            functools.partial(stats_kernel, pops, share, count),
            out_shape=jax.ShapeDtypeStruct((lines + 8, LANES), f32),
            in_specs=[vmem] * (2 * count),
            out_specs=vmem,
            compiler_params=small(4),
            name="stats",
        )(*reads, *totals)
        for bit in gene_bits:
            message = message + swap(message, "gene", n_gene, bit)
        tot = message[lines:]
        for bit in donor_bits:
            tot = tot + swap(tot, "donor", n_donor, bit)

        native_reads = message[: lines // 2].reshape(cells)
        contam_reads = message[lines // 2 : lines].reshape(cells)
        new_theta = (contam_reads + BETA) / (native_reads + contam_reads + 2.0 * BETA)
        ambient_reads = contam_reads / TRANSCRIPT_TOTAL

        widths = tuple(size * TILE for size in sizes)
        new_profiles, new_ambient = pl.pallas_call(
            functools.partial(final_kernel, pops, share, donors, widths, genes, count),
            out_shape=(
                jax.ShapeDtypeStruct((share, genes), f32),
                jax.ShapeDtypeStruct((donors, genes), f32),
            ),
            in_specs=[vmem] + [vmem] * (2 * count),
            out_specs=(vmem, vmem),
            compiler_params=small(8),
            name="final",
        )(tot, *keeps, *last)
        return new_profiles, new_ambient, new_theta, ambient_reads

    in_specs = (
        P("donor", "gene"), P("donor", "gene"), P("donor"), P("donor"), P(), P("donor"),
        P(None, "gene"), P(None, "gene"),
    )
    out_specs = (P("donor", "gene"), P(None, "gene"), P("donor"), P("donor"))
    return jax.shard_map(body, mesh=mesh, in_specs=in_specs, out_specs=out_specs, check_vma=False)
```
